32 devices in a mesh: groups: 2 (over y), expert: 16 (over z, x, core).
Axes of the slice: x: 2, y: 2, z: 4, core: 2. Of those that a mesh axis runs over, the one named last changes fastest.
Arguments:
- attn_heads: bfloat16 [4096, 4096], P(('groups', 'expert')), parts along dimension 0, may hold values from -6 to 6
- residual: bfloat16 [4096, 2048], P(('groups', 'expert')), parts along dimension 0, may hold values from -6 to 6
- w_out: bfloat16 [4096, 2048], P('expert'), may hold values from -0.09375 to 0.09375
- norm_gain: float32 [2048], replicated, may hold values from 0.1 to 1.9
- expert_ids: int32 [4096, 8], P(('groups', 'expert')), parts along dimension 0, may hold values from 0 to 15, all different within a row; in each aligned block of 128 rows (0 to 127, 128 to 255, ...) at most 80 rows name the same one
- route_num: int32 [4096, 8], P(('groups', 'expert')), parts along dimension 0, may hold values from 1 to 16
- w_gate: bfloat16 [16, 2048, 768], P('expert'), may hold values from -0.125 to 0.125
- w_up: bfloat16 [16, 2048, 768], P('expert'), may hold values from -0.125 to 0.125
- w_down: bfloat16 [16, 768, 2048], P('expert'), may hold values from -0.21875 to 0.21875
Outputs:
- mid_state: bfloat16 [4096, 2048], P(('groups', 'expert')), parts along dimension 0
- expert_out: bfloat16 [4096, 2048], P(('groups', 'expert')), parts along dimension 0
The draws below stay inside these ranges and needn't reach their ends.
There are 2 independent parts, one for each index of `groups`. The reference program is written for one: setup_inputs(seed, part) draws one part's arguments, and reference() takes and returns one part's arrays. A program takes and returns all parts, laid end to end along the dimension named above; an argument that names none is the same for every part. Nothing has to cross between parts.
Inputs may be any that keep to these rules, and one draw needn't show every extreme that they name: `expert_ids`: each token names 8 different experts; among the 128 tokens of one device no expert is named more than 80 times, a bound that some block reaches.
All inputs are finite; a program needn't handle non-finite values.
Results may differ from the reference program's by a relative error of at most 0.0095.
Values may be sent and summed in bfloat16 or wider, within the bound.
No kernel may reach another device: no remote copies, remote signals or barrier semaphores. Data moves between devices by JAX's collectives and lax.ppermute only.
A program may use at most 128 MiB of HBM per device.

```python
import math
import jax
import jax.numpy as jnp
import numpy as np
from jax import lax

D = 2048
FFE = 768
TOPK = 8
TOK_DEV = 128
ATT = 4096
TOKENS = 2048
EXPERTS = 16
CAP = 80
N_EXPERT = 16


def plant(entries, own_key, smallest, high):
    longest = entries.shape.index(max(entries.shape))
    spots = []
    for shift in (0, 1):
        where = [jax.random.randint(jax.random.fold_in(own_key, axis), (), 0, length) for axis, length in enumerate(entries.shape)]
        where[longest] = (where[longest] + shift) % entries.shape[longest]
        spots.append(tuple(where))
    return entries.at[spots[0]].set(smallest).at[spots[1]].set(high)


def block_levels(stream_key, dims, cuts, smallest, top_value):
    loudness, own = 1.0, jax.random.fold_in(stream_key, 6)
    for axis_at, shards_of in cuts:
        steps = jnp.exp(jax.random.uniform(jax.random.fold_in(own, axis_at), (shards_of,), jnp.float32, smallest / len(cuts), top_value / len(cuts)))
        loudness = loudness * jnp.repeat(steps, dims[axis_at] // shards_of).reshape([-1 if axis == axis_at else 1 for axis in range(len(dims))])
    return loudness


def routed_block(stream_key, own, number, rows, number_of, top, bound, slope):
    order = jax.random.permutation(stream_key, number_of)
    packed, ordinary = shares(number_of, rows * top, bound, slope, True), shares(number_of, rows * top, bound, slope, False)
    places = jnp.arange(number_of)

    def named(tallies, offset_by):
        used = int((tallies > 0).sum())
        fixed = max(1, used // 4)
        passed = fixed + (places - fixed + offset_by * (used - fixed)) % max(1, number_of - fixed)
        return jnp.zeros((number_of,), jnp.int32).at[order[jnp.where(places < fixed, places, passed)]].set(jnp.asarray(tallies, jnp.int32))

    tallies = jnp.where(number % 4 == 0, named(packed, number // 4), named(ordinary, number - number // 4 - 1))
    mixed = jax.random.permutation(jax.random.fold_in(own, 3), number_of)
    source_of, sink = mixed[0:number_of // 2 * 2:2], mixed[1:number_of // 2 * 2:2]
    margin = jnp.minimum(tallies[source_of] - 1, bound - tallies[sink]) // 2
    margin = jnp.where((source_of == order[0]) | (sink == order[0]) | (tallies[sink] == 0), 0, jnp.maximum(margin, 0))
    passed = jax.random.randint(jax.random.fold_in(own, 4), (number_of // 2,), 0, 1 << 20) % (margin + 1)
    tallies = tallies.at[source_of].add(-passed).at[sink].add(passed)
    labels = jnp.searchsorted(jnp.cumsum(tallies), jnp.arange(rows * top), side="right").astype(jnp.int32)
    grid = labels.reshape(top, rows).T
    grid = grid[jax.random.permutation(jax.random.fold_in(own, 1), rows)]
    offset_by = jax.random.randint(jax.random.fold_in(own, 2), (rows, 1), 0, top)
    return jnp.take_along_axis(grid, (jnp.arange(top)[None, :] + offset_by) % top, axis=1)


def shares(count, total, bound, lean, full):
    loads = [(1 << 20) // math.isqrt(rank ** lean) + 1 for rank in range(1, count + 1)]
    largest = bound if full else min(bound, max(-(-total // count), total * loads[0] // sum(loads)))
    least = 1 if total - largest >= count - 1 else 0
    counts, spare = [largest] + [least] * (count - 1), total - largest - least * (count - 1)
    while spare > 0:
        free = [i for i in range(1, count) if counts[i] < largest] or [i for i in range(1, count) if counts[i] < bound]
        whole, budget = sum([loads[i] for i in free]), spare
        for i in free:
            addition = min(bound - counts[i], max(1, budget * loads[i] // whole), spare)
            counts[i] = counts[i] + addition
            spare = spare - addition
    return np.array(counts)


def scatter_about(key, dims, scale, bound, cuts=(), kind=jnp.bfloat16):
    drawn = scale * jax.random.normal(key, dims, jnp.float32)
    if cuts:
        drawn = drawn * block_levels(key, dims, cuts, -0.22, 0.18)
    return jnp.clip(drawn, -bound, bound).astype(kind)


def setup_inputs(seed: int = 0, part: int = 0) -> dict:
    keys = jax.random.split(jax.random.key(seed), 10)
    part_splits = jax.random.split(jax.random.fold_in(keys[9], part), 10)
    attn_heads = scatter_about(part_splits[0], (TOKENS, ATT), 1.0, 6.0, ((0, 16),))
    residual = scatter_about(part_splits[1], (TOKENS, D), 1.0, 6.0, ((0, 16),))
    w_out = scatter_about(keys[2], (ATT, D), ATT ** -0.5, 0.09375, ((0, 16),))
    norm_gain = jnp.clip(1.0 + 0.18 * jax.random.normal(keys[3], (D,), jnp.float32), 0.1, 1.9)
    expert_ids_keys = jax.random.split(jax.random.fold_in(part_splits[4], 1), TOKENS // TOK_DEV)
    expert_ids_turns = jax.random.permutation(jax.random.fold_in(part_splits[4], 3), TOKENS // TOK_DEV)
    expert_ids = jax.vmap(lambda own, number: routed_block(jax.random.fold_in(part_splits[4], 2), own, number, TOK_DEV, EXPERTS, TOPK, CAP, 2))(expert_ids_keys, expert_ids_turns).reshape((TOKENS, TOPK))
    route_num = plant(jax.random.randint(part_splits[5], (TOKENS, TOPK), 1, 17), jax.random.fold_in(part_splits[5], 1), 1, 16).astype(jnp.int32)
    w_gate = scatter_about(keys[6], (EXPERTS, D, FFE), D ** -0.5, 0.125, ((0, 16),))
    w_up = scatter_about(keys[7], (EXPERTS, D, FFE), D ** -0.5, 0.125, ((0, 16),))
    w_down = scatter_about(keys[8], (EXPERTS, FFE, D), FFE ** -0.5, 0.21875, ((0, 16),))
    return dict(attn_heads=attn_heads, residual=residual, w_out=w_out, norm_gain=norm_gain, expert_ids=expert_ids, route_num=route_num, w_gate=w_gate, w_up=w_up, w_down=w_down)


epsilon = 1e-06

def rms_scale(tensor, norm_gain):
    values = tensor.astype(jnp.float32)
    mean_sq = lax.optimization_barrier(jnp.mean(values * values, axis=-1, keepdims=True))
    return (values * lax.rsqrt(mean_sq + epsilon) * norm_gain).astype(jnp.bfloat16)

def reference(attn_heads, residual, w_out, norm_gain, expert_ids, route_num, w_gate, w_up, w_down):
    projected = jnp.dot(attn_heads, w_out, preferred_element_type=jnp.float32)
    mid_state = (residual.astype(jnp.float32) + projected).astype(jnp.bfloat16)
    normed = rms_scale(mid_state, norm_gain)
    numer = route_num.astype(jnp.float32)
    weights = numer / lax.optimization_barrier(jnp.sum(numer, axis=1, keepdims=True))
    ids_dev = expert_ids.reshape(N_EXPERT, TOK_DEV * TOPK)
    onehot = (ids_dev[:, :, None] == jnp.arange(EXPERTS, dtype=jnp.int32)[None, None, :]).astype(jnp.int32)
    before = jnp.cumsum(onehot, axis=1) - onehot
    slot_index = lax.optimization_barrier(jnp.sum(before * onehot, axis=2))
    device_of = jnp.arange(N_EXPERT, dtype=jnp.int32)[:, None]
    row_index = (device_of * CAP + slot_index).reshape(-1).astype(jnp.int32)
    flat_ids = expert_ids.reshape(-1)
    token_index = jnp.arange(TOKENS * TOPK, dtype=jnp.int32) // TOPK
    token_of_row = jnp.full((EXPERTS, N_EXPERT * CAP), TOKENS, jnp.int32).at[flat_ids, row_index].set(token_index)
    weight_of_row = jnp.zeros((EXPERTS, N_EXPERT * CAP), jnp.float32).at[flat_ids, row_index].set(weights.reshape(-1))
    padded = jnp.concatenate([normed, jnp.zeros((1, D), jnp.bfloat16)], axis=0)

    def one_expert(running, inputs):
        gate_mat, up_mat, down_mat, token_rows, row_weights = inputs
        row_block = padded[token_rows]
        gate_act = jnp.dot(row_block, gate_mat, preferred_element_type=jnp.float32)
        up_act = jnp.dot(row_block, up_mat, preferred_element_type=jnp.float32)
        hidden = (jax.nn.silu(gate_act) * up_act).astype(jnp.bfloat16)
        result = jnp.dot(hidden, down_mat, preferred_element_type=jnp.float32).astype(jnp.bfloat16)
        running = running.at[token_rows].add(row_weights[:, None] * result.astype(jnp.float32))
        return (running, None)
    start = jnp.zeros((TOKENS + 1, D), jnp.float32)
    running, _ = lax.scan(one_expert, start, (w_gate, w_up, w_down, token_of_row, weight_of_row))
    expert_out = running[:TOKENS].astype(jnp.bfloat16)
    return (mid_state, expert_out)
```

```python
import functools

import jax
import jax.numpy as jnp
import numpy as np
from jax import lax
from jax.experimental import pallas as pl
from jax.experimental.pallas import tpu as pltpu
from jax.sharding import PartitionSpec as P

epsilon = 1e-06


def rms_scale(tensor, norm_gain):
    values = tensor.astype(jnp.float32)
    mean_sq = jnp.mean(values * values, axis=-1, keepdims=True)
    return (values * lax.rsqrt(mean_sq + epsilon) * norm_gain).astype(jnp.bfloat16)


def sparse_device(attn_heads, residual, w_out, norm_gain, expert_ids, route_num, w_gate, w_up, w_down):
    tok_rows = attn_heads.shape[0]
    feature_count = residual.shape[1]
    gathered = lax.all_gather(w_out, "expert", axis=0, tiled=True)
    projected = jnp.dot(attn_heads, gathered, preferred_element_type=jnp.float32)
    mid_state = (residual.astype(jnp.float32) + projected).astype(jnp.bfloat16)
    n_experts = lax.axis_size("expert")
    top_count = expert_ids.shape[1]
    capacity = tok_rows * top_count * 5 // (4 * n_experts)
    flat_ids = expert_ids.reshape(-1)
    onehot = (flat_ids[:, None] == jnp.arange(n_experts, dtype=jnp.int32)[None, :]).astype(
        jnp.int32
    )
    before = jnp.cumsum(onehot, axis=0) - onehot
    slot_index = jnp.sum(before * onehot, axis=1)
    position = flat_ids * capacity + slot_index
    token_index = jnp.arange(tok_rows * top_count, dtype=jnp.int32) // top_count
    payload = rms_scale(mid_state, norm_gain)
    sendbuf = jnp.zeros((n_experts * capacity, feature_count), jnp.bfloat16)
    sendbuf = sendbuf.at[position].set(payload[token_index])
    sendbuf = sendbuf.reshape(n_experts, capacity, feature_count)
    received = lax.all_to_all(sendbuf, "expert", split_axis=0, concat_axis=0, tiled=True)
    sources, slot_count, _ = received.shape
    row_block = received.reshape(sources * slot_count, feature_count)
    gate_act = jnp.dot(row_block, w_gate[0], preferred_element_type=jnp.float32)
    up_act = jnp.dot(row_block, w_up[0], preferred_element_type=jnp.float32)
    hidden = (jax.nn.silu(gate_act) * up_act).astype(jnp.bfloat16)
    result = jnp.dot(hidden, w_down[0], preferred_element_type=jnp.float32).astype(jnp.bfloat16)
    result = result.reshape(sources, slot_count, feature_count)
    returned = lax.all_to_all(result, "expert", split_axis=0, concat_axis=0, tiled=True)
    returned = returned.reshape(n_experts * capacity, feature_count)
    picked = returned[position].astype(jnp.float32).reshape(tok_rows, top_count, feature_count)
    numer = route_num.astype(jnp.float32)
    weights = numer / jnp.sum(numer, axis=1, keepdims=True)
    expert_out = jnp.sum(picked * weights[:, :, None], axis=1).astype(jnp.bfloat16)
    return (mid_state, expert_out)


def chip_ring(mesh):
    row = mesh.devices.reshape(mesh.shape["groups"], mesh.shape["expert"])[0]
    chips = {}
    for index, device in enumerate(row):
        chips.setdefault(tuple(device.coords), []).append(index)
    spots = sorted(chips)
    spans = [sorted({spot[axis] for spot in spots}) for axis in range(len(spots[0]))]
    across = min((axis for axis in range(len(spans)) if len(spans[axis]) > 1), key=lambda axis: len(spans[axis]))
    walk = []
    for turn, value in enumerate(spans[across]):
        column = [spot for spot in spots if spot[across] == value]
        walk += column if turn % 2 == 0 else column[::-1]
    return [[chips[spot][core] for spot in walk] for core in range(2)]


def reorder_kernel(place_ref, wide_ref, mine_ref, send_ref):
    block = mine_ref.shape[1] // (place_ref.shape[0] // 2)
    for part, out_ref in enumerate((mine_ref, send_ref)):
        count = place_ref.shape[0] // 2
        for k in range(count):
            at = pl.multiple_of(place_ref[part * count + k] * block, block)
            out_ref[:, k * block : (k + 1) * block] = wide_ref[:, pl.ds(at, block)]


def reorder(places, wide):
    half = jax.ShapeDtypeStruct((wide.shape[0], wide.shape[1] // 2), wide.dtype)
    vmem = pl.BlockSpec(memory_space=pltpu.VMEM)
    return pl.pallas_call(
        reorder_kernel,
        out_shape=(half, half),
        in_specs=[pl.BlockSpec(memory_space=pltpu.SMEM), vmem],
        out_specs=(vmem, vmem),
        cost_estimate=pl.CostEstimate(flops=wide.size, bytes_accessed=4 * wide.size, transcendentals=0),
        name="reorder",
    )(places, wide)


def project_kernel(chunk_count, pieces, has_total, last, *refs):
    mine_ref, near_ref = refs[:2]
    w_refs = refs[2 : 2 + chunk_count * pieces]
    refs = refs[2 + chunk_count * pieces :]
    if has_total:
        total_ref, refs = refs[0], refs[1:]
    rows = mine_ref.shape[0]
    block = w_refs[0].shape[0]
    width = w_refs[0].shape[1]
    for side, heads_ref in enumerate((mine_ref, near_ref)):
        for piece in range(pieces):
            columns = slice(piece * width, (piece + 1) * width)
            value = total_ref[side * rows : (side + 1) * rows, columns] if has_total else None
            for k in range(chunk_count):
                part = jnp.dot(
                    heads_ref[:, k * block : (k + 1) * block],
                    w_refs[k * pieces + piece][...],
                    preferred_element_type=jnp.float32,
                )
                value = part if value is None else value + part
            if not last:
                refs[0][side * rows : (side + 1) * rows, columns] = value
            elif side == 0:
                refs[0][:, columns] = value
            else:
                count = len(refs) - 1
                for i in range(count):
                    rows_i = rows // count
                    refs[1 + i][:, columns] = value[i * rows_i : (i + 1) * rows_i].astype(jnp.bfloat16)


def project(mine, near, chunks, total, last):
    pieces = len(chunks[0])
    rows, depth = mine.shape
    features = pieces * chunks[0][0].shape[1]
    flat = [piece for chunk in chunks for piece in chunk]
    if last:
        out_shape = [jax.ShapeDtypeStruct((rows, features), jnp.float32)]
        out_shape += [jax.ShapeDtypeStruct((rows // 2, features), jnp.bfloat16)] * 2
    else:
        out_shape = [jax.ShapeDtypeStruct((2 * rows, features), jnp.float32)]
    operands = [mine, near] + flat + ([] if total is None else [total])
    vmem = pl.BlockSpec(memory_space=pltpu.VMEM)
    alias = {} if total is None or last else {len(operands) - 1: 0}
    return pl.pallas_call(
        functools.partial(project_kernel, len(chunks), pieces, total is not None, last),
        out_shape=out_shape,
        in_specs=[vmem] * len(operands),
        out_specs=[vmem] * len(out_shape),
        input_output_aliases=alias,
        cost_estimate=pl.CostEstimate(
            flops=4 * rows * depth * features,
            bytes_accessed=2 * depth * features + 16 * rows * features,
            transcendentals=0,
        ),
        name="project",
    )(*operands)


def ring_device(lanes, attn_heads, residual, w_out, norm_gain, expert_ids, route_num, w_gate, w_up, w_down):
    n_experts = lax.axis_size("expert")
    chips = len(lanes[0])
    half = chips // 2
    expert = lax.axis_index("expert")
    group = lax.axis_index("groups")
    rows, features = residual.shape
    shard = w_out.shape[0]
    block = shard // 2

    def shift(step):
        pairs = [(lane[p], lane[(p + step) % chips]) for lane in lanes for p in range(chips)]
        return lambda value: lax.ppermute(value, "expert", pairs)

    right, left = shift(1), shift(-1)
    swap_pairs = [(lanes[c][p], lanes[1 - c][p]) for c in range(2) for p in range(chips)]
    swap = lambda value: lax.ppermute(value, "expert", swap_pairs)
    across = lambda value: lax.ppermute(value, "groups", [(0, 1), (1, 0)])

    order = np.zeros((n_experts, n_experts), np.int32)
    partner = np.zeros((n_experts,), np.int32)
    for c in range(2):
        for p in range(chips):
            spots = [(0, c), (0, 1 - c)]
            for d in range(1, half):
                spots += [(-d, c), (d, c), (-d, 1 - c), (d, 1 - c)]
            spots += [(half, c), (half, 1 - c)]
            order[lanes[c][p]] = [lanes[lane][(p + d) % chips] for d, lane in spots]
            partner[lanes[c][p]] = lanes[1 - c][p]
    order = lax.dynamic_index_in_dim(jnp.asarray(order), expert, keepdims=False)
    other = lax.dynamic_index_in_dim(jnp.asarray(partner), expert, keepdims=False)

    piece_width = features // 2
    pieces = [
        lax.dynamic_slice(w_out, (group * block, i * piece_width), (block, piece_width)) for i in range(2)
    ]
    places = jnp.concatenate([2 * order + group, 2 * order + 1 - group])
    mine, send = reorder(places, attn_heads)

    numer = route_num.astype(jnp.float32)
    weights = numer / jnp.sum(numer, axis=1, keepdims=True)
    dense = jnp.sum(
        jnp.where(expert_ids.T[None, :, :] == jnp.arange(n_experts, dtype=jnp.int32)[:, None, None], weights.T[None], 0.0),
        axis=1,
    )

    near = across(send)
    to_right, to_left = list(pieces), list(pieces)
    route_right = route_left = dense
    routes = {0: dense}
    experts_near = [swap(w[0]) for w in (w_gate, w_up, w_down)]
    total = project(mine[:, : 2 * block], near[:, : 2 * block], [pieces, [swap(v) for v in pieces]], None, False)[0]
    at = 2 * block
    for d in range(1, half):
        to_right = [right(v) for v in to_right]
        to_left = [left(v) for v in to_left]
        route_right, route_left = right(route_right), left(route_left)
        routes[-d], routes[d] = route_right, route_left
        chunks = [to_right, to_left, [swap(v) for v in to_right], [swap(v) for v in to_left]]
        columns = slice(at, at + 4 * block)
        total = project(mine[:, columns], near[:, columns], chunks, total, False)[0]
        at += 4 * block
    final = [right(to_right[0]), left(to_left[1])]
    routes[half] = left(route_left)
    own, back0, back1 = project(
        mine[:, at:], near[:, at:], [final, [swap(v) for v in final]], total, True
    )
    back = [across(back0), across(back1)]
    sub = rows // 2
    mids, normed = [], []
    for i in range(2):
        part = slice(i * sub, (i + 1) * sub)
        mid = (residual[part].astype(jnp.float32) + own[part] + back[i].astype(jnp.float32)).astype(jnp.bfloat16)
        mids.append(mid)
        normed.append(rms_scale(mid, norm_gain))
    mid_state = jnp.concatenate(mids, axis=0)

    def routed(d):
        pair = [lax.dynamic_index_in_dim(routes[d], e, keepdims=False) for e in (expert, other)]
        return pair

    gates, ups, downs = ([w[0], w_near] for w, w_near in zip((w_gate, w_up, w_down), experts_near))

    def run_experts(tokens, scale):
        result = None
        for i in range(2):
            gate_act = jnp.dot(tokens, gates[i], preferred_element_type=jnp.float32)
            up_act = jnp.dot(tokens, ups[i], preferred_element_type=jnp.float32)
            hidden = (jax.nn.silu(gate_act) * up_act * scale[i][:, None]).astype(jnp.bfloat16)
            part = jnp.dot(hidden, downs[i], preferred_element_type=jnp.float32)
            result = part if result is None else result + part
        return result.astype(jnp.bfloat16)

    scales = {d: routed(d) for d in routes}
    to_right, to_left = list(normed), list(normed)
    out = {}
    value = run_experts(jnp.concatenate(normed, axis=0), scales[0])
    out[0] = [value[:sub], value[sub:]]
    for d in range(1, half):
        to_right = [right(v) for v in to_right]
        to_left = [left(v) for v in to_left]
        value = run_experts(
            jnp.concatenate(to_right + to_left, axis=0),
            [jnp.concatenate([a, b]) for a, b in zip(scales[-d], scales[d])],
        )
        parts = [value[i * sub : (i + 1) * sub] for i in range(4)]
        out[-d], out[d] = parts[:2], parts[2:]
    final = [right(to_right[0]), left(to_left[1])]
    value = run_experts(jnp.concatenate(final, axis=0), scales[half])
    far = [value[:sub], value[sub:]]

    def add(a, b):
        return (a.astype(jnp.float32) + b.astype(jnp.float32)).astype(jnp.bfloat16)

    go_right = [out[half - 1][0], add(out[half - 1][1], right(far[1]))]
    go_left = [add(out[1 - half][0], left(far[0])), out[1 - half][1]]
    for d in range(half - 2, 0, -1):
        go_right = [add(a, right(b)) for a, b in zip(out[d], go_right)]
        go_left = [add(a, left(b)) for a, b in zip(out[-d], go_left)]
    parts = []
    for i in range(2):
        parts.append(
            (
                out[0][i].astype(jnp.float32)
                + right(go_right[i]).astype(jnp.float32)
                + left(go_left[i]).astype(jnp.float32)
            ).astype(jnp.bfloat16)
        )
    return (mid_state, jnp.concatenate(parts, axis=0))


def solution(mesh):
    in_specs = (
        P(("groups", "expert"), None),
        P(("groups", "expert"), None),
        P("expert", None),
        P(),
        P(("groups", "expert"), None),
        P(("groups", "expert"), None),
        P("expert", None, None),
        P("expert", None, None),
        P("expert", None, None),
    )
    out_specs = (P(("groups", "expert"), None), P(("groups", "expert"), None))

    def whole(*args):
        n_experts, top_count = mesh.shape["expert"], args[4].shape[1]
        if mesh.shape["groups"] == 2 and n_experts <= 2 * top_count:
            per_device = functools.partial(ring_device, chip_ring(mesh))
        else:
            per_device = sparse_device
        return jax.shard_map(
            per_device, mesh=mesh, in_specs=in_specs, out_specs=out_specs, check_vma=False
        )(*args)

    return whole
```

```python
import functools

import jax
import jax.numpy as jnp
import numpy as np
from jax import lax
from jax.experimental import pallas as pl
from jax.experimental.pallas import tpu as pltpu
from jax.sharding import PartitionSpec as P

epsilon = 1e-06


def rms_scale(tensor, norm_gain):
    values = tensor.astype(jnp.float32)
    mean_sq = jnp.mean(values * values, axis=-1, keepdims=True)
    return (values * lax.rsqrt(mean_sq + epsilon) * norm_gain).astype(jnp.bfloat16)


def sparse_device(attn_heads, residual, w_out, norm_gain, expert_ids, route_num, w_gate, w_up, w_down):
    tok_rows = attn_heads.shape[0]
    feature_count = residual.shape[1]
    gathered = lax.all_gather(w_out, "expert", axis=0, tiled=True)
    projected = jnp.dot(attn_heads, gathered, preferred_element_type=jnp.float32)
    mid_state = (residual.astype(jnp.float32) + projected).astype(jnp.bfloat16)
    n_experts = lax.axis_size("expert")
    top_count = expert_ids.shape[1]
    capacity = tok_rows * top_count * 5 // (4 * n_experts)
    flat_ids = expert_ids.reshape(-1)
    onehot = (flat_ids[:, None] == jnp.arange(n_experts, dtype=jnp.int32)[None, :]).astype(
        jnp.int32
    )
    before = jnp.cumsum(onehot, axis=0) - onehot
    slot_index = jnp.sum(before * onehot, axis=1)
    position = flat_ids * capacity + slot_index
    token_index = jnp.arange(tok_rows * top_count, dtype=jnp.int32) // top_count
    payload = rms_scale(mid_state, norm_gain)
    sendbuf = jnp.zeros((n_experts * capacity, feature_count), jnp.bfloat16)
    sendbuf = sendbuf.at[position].set(payload[token_index])
    sendbuf = sendbuf.reshape(n_experts, capacity, feature_count)
    received = lax.all_to_all(sendbuf, "expert", split_axis=0, concat_axis=0, tiled=True)
    sources, slot_count, _ = received.shape
    row_block = received.reshape(sources * slot_count, feature_count)
    gate_act = jnp.dot(row_block, w_gate[0], preferred_element_type=jnp.float32)
    up_act = jnp.dot(row_block, w_up[0], preferred_element_type=jnp.float32)
    hidden = (jax.nn.silu(gate_act) * up_act).astype(jnp.bfloat16)
    result = jnp.dot(hidden, w_down[0], preferred_element_type=jnp.float32).astype(jnp.bfloat16)
    result = result.reshape(sources, slot_count, feature_count)
    returned = lax.all_to_all(result, "expert", split_axis=0, concat_axis=0, tiled=True)
    returned = returned.reshape(n_experts * capacity, feature_count)
    picked = returned[position].astype(jnp.float32).reshape(tok_rows, top_count, feature_count)
    numer = route_num.astype(jnp.float32)
    weights = numer / jnp.sum(numer, axis=1, keepdims=True)
    expert_out = jnp.sum(picked * weights[:, :, None], axis=1).astype(jnp.bfloat16)
    return (mid_state, expert_out)


def chip_ring(mesh):
    row = mesh.devices.reshape(mesh.shape["groups"], mesh.shape["expert"])[0]
    chips = {}
    for index, device in enumerate(row):
        chips.setdefault(tuple(device.coords), []).append(index)
    spots = sorted(chips)
    spans = [sorted({spot[axis] for spot in spots}) for axis in range(len(spots[0]))]
    across = min((axis for axis in range(len(spans)) if len(spans[axis]) > 1), key=lambda axis: len(spans[axis]))
    walk = []
    for turn, value in enumerate(spans[across]):
        column = [spot for spot in spots if spot[across] == value]
        walk += column if turn % 2 == 0 else column[::-1]
    return [[chips[spot][core] for spot in walk] for core in range(2)]


def reorder_kernel(table_ref, wide_ref, mine_ref, send_ref):
    device, group = lax.axis_index("expert"), lax.axis_index("groups")
    count = table_ref.shape[1]
    block = mine_ref.shape[1] // count
    for out_ref, side in ((mine_ref, group), (send_ref, 1 - group)):
        for k in range(count):
            at = pl.multiple_of((2 * table_ref[device, k] + side) * block, block)
            out_ref[:, k * block : (k + 1) * block] = wide_ref[:, pl.ds(at, block)]


def reorder(table, wide):
    half = jax.ShapeDtypeStruct((wide.shape[0], wide.shape[1] // 2), wide.dtype)
    vmem = pl.BlockSpec(memory_space=pltpu.VMEM)
    return pl.pallas_call(
        reorder_kernel,
        out_shape=(half, half),
        in_specs=[pl.BlockSpec(memory_space=pltpu.SMEM), vmem],
        out_specs=(vmem, vmem),
        cost_estimate=pl.CostEstimate(flops=wide.size, bytes_accessed=4 * wide.size, transcendentals=0),
        compiler_params=pltpu.CompilerParams(vmem_limit_bytes=8 << 20),
        name="reorder",
    )(table, wide)


def project_kernel(at, first_row, steps, has_total, narrow, *refs):
    heads, refs = refs[: len(first_row)], refs[len(first_row) :]
    w_refs, refs = refs[:steps], refs[steps:]
    if has_total:
        total_ref, refs = refs[0], refs[1:]
    block, features = w_refs[0].shape
    rows = heads[0].shape[0]
    width = features // 2
    for side, heads_ref in enumerate(heads):
        here = slice(side * rows, (side + 1) * rows)
        there = slice(first_row[side], first_row[side] + rows)
        for piece in range(2):
            columns = slice(piece * width, (piece + 1) * width)
            value = total_ref[there, columns] if has_total else None
            for k in range(steps):
                part = jnp.dot(
                    heads_ref[:, at + k * block : at + (k + 1) * block],
                    w_refs[k][:, columns],
                    preferred_element_type=jnp.float32,
                )
                value = part if value is None else value + part
            refs[0][here, columns] = value.astype(refs[0].dtype)


def project(heads, first_row, at, chunks, total, dtype=jnp.float32):
    rows = heads[0].shape[0]
    features = chunks[0].shape[1]
    depth = len(chunks) * chunks[0].shape[0]
    out_shape = jax.ShapeDtypeStruct((len(heads) * rows, features), dtype)
    operands = [*heads, *chunks] + ([] if total is None else [total])
    vmem = pl.BlockSpec(memory_space=pltpu.VMEM)
    alias = {len(operands) - 1: 0} if total is not None and len(heads) == 2 else {}
    return pl.pallas_call(
        functools.partial(project_kernel, at, first_row, len(chunks), total is not None, dtype != jnp.float32),
        out_shape=out_shape,
        in_specs=[vmem] * len(operands),
        out_specs=vmem,
        input_output_aliases=alias,
        cost_estimate=pl.CostEstimate(
            flops=2 * len(heads) * rows * depth * features,
            bytes_accessed=2 * depth * features + 8 * len(heads) * rows * features,
            transcendentals=0,
        ),
        compiler_params=pltpu.CompilerParams(vmem_limit_bytes=16 << 20),
        name="project",
    )(*operands)


def normalize_kernel(own_ref, back_ref, residual_ref, gain_ref, ids_ref, numer_ref, mid_ref, tokens_ref):
    features = own_ref.shape[1]
    mid = (residual_ref[...].astype(jnp.float32) + own_ref[...] + back_ref[...].astype(jnp.float32)).astype(jnp.bfloat16)
    mid_ref[...] = mid
    tokens_ref[:, :features] = rms_scale(mid, gain_ref[...])
    lane = lax.broadcasted_iota(jnp.int32, (own_ref.shape[0], tokens_ref.shape[1] - features), 1)
    dense = jnp.zeros(lane.shape, jnp.float32)
    numer = numer_ref[...].astype(jnp.float32)
    for k in range(ids_ref.shape[1]):
        dense += jnp.where(ids_ref[:, k : k + 1] == lane, numer[:, k : k + 1], 0.0)
    tokens_ref[:, features:] = dense.astype(jnp.bfloat16)


def normalize(own, back, residual, norm_gain, expert_ids, route_num, n_experts):
    rows, features = residual.shape
    extra = -(-n_experts // 128) * 128
    vmem = pl.BlockSpec(memory_space=pltpu.VMEM)
    return pl.pallas_call(
        normalize_kernel,
        out_shape=(
            jax.ShapeDtypeStruct((rows, features), jnp.bfloat16),
            jax.ShapeDtypeStruct((rows, features + extra), jnp.bfloat16),
        ),
        in_specs=[vmem] * 6,
        out_specs=(vmem, vmem),
        cost_estimate=pl.CostEstimate(flops=10 * rows * features, bytes_accessed=12 * rows * features, transcendentals=rows),
        compiler_params=pltpu.CompilerParams(vmem_limit_bytes=12 << 20),
        name="normalize",
    )(own, back, residual, norm_gain.reshape(1, -1), expert_ids, route_num)


def experts_kernel(count, tile, out_tile, partner_ref, *refs):
    tokens, weights, outs = refs[:count], refs[count : count + 6], refs[count + 6 : 2 * count + 6]
    x_ref, hidden_ref, out_ref, *held = refs[2 * count + 6 : 2 * count + 15]
    token_sem, gate_sem, down_sem, out_sem = refs[2 * count + 15 :]
    rows = tokens[0].shape[0]
    features = out_ref.shape[1]
    depth = weights[0].shape[1]
    tiles, out_tiles = depth // tile, features // out_tile

    token_copies = [
        pltpu.make_async_copy(tokens[i], x_ref.at[i * rows : (i + 1) * rows], token_sem.at[i]) for i in range(count)
    ]
    for copy in token_copies:
        copy.start()
    gate_copies, down_copies = [], []
    for e in range(2):
        for t in range(tiles):
            columns = slice(t * tile, (t + 1) * tile)
            for k in range(2):
                copy = pltpu.make_async_copy(
                    weights[3 * e + k].at[:, columns], held[3 * e + k].at[:, columns], gate_sem.at[e, t, k]
                )
                copy.start()
                gate_copies.append(copy)
    for n in range(out_tiles):
        columns = slice(n * out_tile, (n + 1) * out_tile)
        for e in range(2):
            copy = pltpu.make_async_copy(
                weights[3 * e + 2].at[:, columns], held[3 * e + 2].at[:, columns], down_sem.at[e, n]
            )
            copy.start()
            down_copies.append(copy)

    for copy in token_copies:
        copy.wait()
    device = lax.axis_index("expert")
    numer = x_ref[:, features:].astype(jnp.float32)
    lane = lax.broadcasted_iota(jnp.int32, numer.shape, 1)
    denom = jnp.sum(numer, axis=1, keepdims=True)
    x = x_ref.at[:, :features]
    for e, expert in enumerate((device, partner_ref[device])):
        scale = jnp.sum(jnp.where(lane == expert, numer, 0.0), axis=1, keepdims=True) / denom
        for t in range(tiles):
            columns = slice(t * tile, (t + 1) * tile)
            for k in range(2):
                gate_copies[(e * tiles + t) * 2 + k].wait()
            gate_act = jnp.dot(x[...], held[3 * e][:, columns], preferred_element_type=jnp.float32)
            up_act = jnp.dot(x[...], held[3 * e + 1][:, columns], preferred_element_type=jnp.float32)
            hidden = gate_act / (1.0 + jnp.exp(-gate_act)) * up_act * scale
            hidden_ref[:, e * depth + t * tile : e * depth + (t + 1) * tile] = hidden.astype(jnp.bfloat16)
    out_copies = []
    for n in range(out_tiles):
        columns = slice(n * out_tile, (n + 1) * out_tile)
        for e in range(2):
            down_copies[n * 2 + e].wait()
        value = jnp.dot(hidden_ref[:, :depth], held[2][:, columns], preferred_element_type=jnp.float32)
        value += jnp.dot(hidden_ref[:, depth:], held[5][:, columns], preferred_element_type=jnp.float32)
        out_ref[:, columns] = value.astype(jnp.bfloat16)
        for i in range(count):
            copy = pltpu.make_async_copy(
                out_ref.at[i * rows : (i + 1) * rows, columns], outs[i].at[:, columns], out_sem.at[i, n]
            )
            copy.start()
            out_copies.append(copy)
    for copy in out_copies:
        copy.wait()


def run_experts(tokens, partner, weights):
    rows, wide = tokens[0].shape
    count = len(tokens)
    features, depth = weights[0].shape
    tile = depth // 3 if depth % 384 == 0 else depth
    out_tile = features // 4 if features % 512 == 0 else features
    anywhere = pl.BlockSpec(memory_space=pltpu.HBM)
    total_rows = count * rows
    return pl.pallas_call(
        functools.partial(experts_kernel, count, tile, out_tile),
        out_shape=[jax.ShapeDtypeStruct((rows, features), jnp.bfloat16)] * count,
        in_specs=[pl.BlockSpec(memory_space=pltpu.SMEM)] + [anywhere] * (count + 6),
        out_specs=[anywhere] * count,
        scratch_shapes=[
            pltpu.VMEM((total_rows, wide), jnp.bfloat16),
            pltpu.VMEM((total_rows, 2 * depth), jnp.bfloat16),
            pltpu.VMEM((total_rows, features), jnp.bfloat16),
            *[pltpu.VMEM(w.shape, jnp.bfloat16) for w in weights],
            pltpu.SemaphoreType.DMA((count,)),
            pltpu.SemaphoreType.DMA((2, depth // tile, 2)),
            pltpu.SemaphoreType.DMA((2, features // out_tile)),
            pltpu.SemaphoreType.DMA((count, features // out_tile)),
        ],
        cost_estimate=pl.CostEstimate(
            flops=12 * total_rows * features * depth,
            bytes_accessed=4 * total_rows * features + 12 * features * depth,
            transcendentals=2 * total_rows * depth,
        ),
        compiler_params=pltpu.CompilerParams(vmem_limit_bytes=40 << 20),
        name="experts",
    )(partner, *tokens, *weights)


def ring_device(lanes, attn_heads, residual, w_out, norm_gain, expert_ids, route_num, w_gate, w_up, w_down):
    n_experts = lax.axis_size("expert")
    chips = len(lanes[0])
    half = chips // 2
    rows, features = residual.shape
    block = w_out.shape[0] // 2

    def hop(step, change):
        turn = (step, -step)
        pairs = [
            (lanes[c][p], lanes[1 - c if change else c][(p + turn[c ^ change if step > 0 else c]) % chips])
            for c in range(2)
            for p in range(chips)
        ]
        return lambda value: lax.ppermute(value, "expert", pairs)

    swap, across = hop(0, 1), lambda value: lax.ppermute(value, "groups", [(0, 1), (1, 0)])
    onward, onward_change = hop(1, 0), hop(1, 1)
    backward, backward_change = hop(-1, 0), hop(-1, 1)

    table = np.zeros((n_experts, n_experts), np.int32)
    partner = np.zeros((n_experts,), np.int32)
    for c in range(2):
        for p in range(chips):
            sign = 2 * c - 1
            spots = [(0, c), (0, 1 - c)]
            for d in range(1, half):
                spots += [(sign * d, c), (sign * d, 1 - c), (-sign * d, 1 - c), (-sign * d, c)]
            spots += [(half, c), (half, 1 - c)]
            table[lanes[c][p]] = [lanes[lane][(p + d) % chips] for d, lane in spots]
            partner[lanes[c][p]] = lanes[1 - c][p]
    table, partner = jnp.asarray(table), jnp.asarray(partner)

    def after(values, *others):
        flat, tree = jax.tree.flatten(values)
        return jax.tree.unflatten(tree, lax.optimization_barrier((*flat, *others))[: len(flat)])

    shard = lax.dynamic_slice_in_dim(w_out, lax.axis_index("groups") * block, block)
    same, other = onward(shard), onward_change(shard)
    arrived = [shard, swap(shard)]
    mine, send = reorder(table, attn_heads)
    near = across(send)
    experts_near = [swap(w[0]) for w in (w_gate, w_up, w_down)]
    heads, both = (mine, near), (0, rows)
    total, at = None, 0
    for d in range(1, half):
        total = project(heads, both, at, arrived, total)
        at += len(arrived) * block
        same, other = after((same, other), total)
        arrived = [same, other, swap(same), swap(other)]
        same, other = onward(same), onward(other) if d < half - 1 else None
    total = project(heads, both, at, arrived, total)
    at += len(arrived) * block
    same = after(same, total)
    arrived = [same, swap(same)]
    back = across(project((near,), (rows,), at, arrived, total, jnp.bfloat16))
    own = project((mine,), (0,), at, arrived, total)
    mid_state, tokens = normalize(own, back, residual, norm_gain, expert_ids, route_num, n_experts)

    weights = [w[0] for w in (w_gate, w_up, w_down)] + experts_near
    same, other = onward(tokens), onward_change(tokens)
    here = run_experts([tokens], partner, weights)
    out = {}
    same, other = after((same, other), here[0])
    for d in range(1, half):
        work = [same, other]
        same, other = onward(same), onward(other) if d < half - 1 else None
        out[d] = run_experts(work, partner, weights)
        same, other = after((same, other), out[d][0])

    def add(a, b):
        return (a.astype(jnp.float32) + b.astype(jnp.float32)).astype(jnp.bfloat16)

    other = backward(out[half - 1][1])
    same = backward(run_experts([same], partner, weights)[0])
    for d in range(half - 1, 0, -1):
        if d < half - 1:
            other = (backward if d > 1 else backward_change)(add(out[d][1], other))
        same = backward(add(out[d][0], same))
    expert_out = here[0].astype(jnp.float32) + same.astype(jnp.float32) + other.astype(jnp.float32)
    return (mid_state, expert_out.astype(jnp.bfloat16))


def solution(mesh):
    in_specs = (
        P(("groups", "expert"), None),
        P(("groups", "expert"), None),
        P("expert", None),
        P(),
        P(("groups", "expert"), None),
        P(("groups", "expert"), None),
        P("expert", None, None),
        P("expert", None, None),
        P("expert", None, None),
    )
    out_specs = (P(("groups", "expert"), None), P(("groups", "expert"), None))

    def whole(*args):
        n_experts, top_count = mesh.shape["expert"], args[4].shape[1]
        if mesh.shape["groups"] == 2 and n_experts <= 2 * top_count:
            per_device = functools.partial(ring_device, chip_ring(mesh))
        else:
            per_device = sparse_device
        return jax.shard_map(
            per_device, mesh=mesh, in_specs=in_specs, out_specs=out_specs, check_vma=False
        )(*args)

    return whole
```
